32 devices in a mesh: row: 8 (over y, x, core), col: 4 (over z).
Axes of the slice: x: 2, y: 2, z: 4, core: 2. Of those that a mesh axis runs over, the one named last changes fastest.
Arguments:
- query: bfloat16 [8, 512, 4096], P(None, 'col'), may hold values from -7 to 7
- key: bfloat16 [4096, 512], P(('row', 'col')), may hold values from -7 to 7
- value: bfloat16 [4096, 512], P(('row', 'col')), may hold values from -4 to 4
- span_order: int32 [32], replicated, may hold values from 0 to 31, each once
Outputs:
- attention: bfloat16 [4096, 4096], P(('row', 'col'))
The draws below stay inside these ranges and needn't reach their ends.
Inputs may be any that keep to these rules, and one draw needn't show every extreme that they name: span_order is a permutation of 0 to 31.
All inputs are finite; a program needn't handle non-finite values.
Results may differ from the reference program's by a relative error of at most 0.0085.
Values may be sent and summed in bfloat16 or wider, within the bound.
A program may use at most 192 MiB of HBM per device.

```python
import jax
import jax.numpy as jnp
from jax import lax

HEAD_DIM = 128
QHEADS = 32
KVHEADS = 4
TOK_DEV = 128
GROUP_ROWS = 512
SPANS = 32
SEQ = 4096


def draw_pair(key):
    first = jax.random.fold_in(key, 101)
    second = jax.random.fold_in(key, 202)
    key_part = jnp.clip(1.75 * jax.random.normal(first, (SEQ, KVHEADS * HEAD_DIM), jnp.float32), -7.0, 7.0)
    query_part = jnp.clip(1.75 * jax.random.normal(second, (SEQ, QHEADS * HEAD_DIM), jnp.float32), -7.0, 7.0)
    return (query_part, key_part)


def draw_query(key, part):
    query_part, unused = draw_pair(key)
    return query_part.reshape(SEQ // GROUP_ROWS, GROUP_ROWS, QHEADS * HEAD_DIM).astype(jnp.bfloat16)


def draw_key(key, part):
    unused, key_part = draw_pair(key)
    return key_part.astype(jnp.bfloat16)


def shard_levels(stream_key, extent, pieces, smallest, high):
    def one(dim, parts):
        draws = jax.random.uniform(jax.random.fold_in(jax.random.fold_in(stream_key, 6), dim), (parts,), jnp.float32, smallest / len(pieces), high / len(pieces))
        return jnp.repeat(jnp.exp(draws), extent[dim] // parts).reshape((-1,) + (1,) * (len(extent) - dim - 1))

    level = one(*pieces[0])
    for cut in pieces[1:]:
        level = level * one(*cut)
    return level


def scatter_about(rng, dims, scale, bound, shards=(), kind=jnp.bfloat16):
    factor_of = shard_levels(rng, dims, shards, -0.22, 0.18) if shards else 1.0
    array = jax.random.normal(rng, dims, jnp.float32) * scale * factor_of
    return jnp.minimum(jnp.maximum(array, -bound), bound).astype(kind)


def setup_inputs(seed: int = 0) -> dict:
    seeds = jax.random.split(jax.random.key(seed), 5)
    query = draw_query(jax.random.fold_in(seeds[4], 71), 0)
    key = draw_key(jax.random.fold_in(seeds[4], 71), 0)
    value = scatter_about(seeds[2], (SEQ, KVHEADS * HEAD_DIM), 1.0, 4.0, ((0, 32),))
    span_order = jax.random.permutation(seeds[3], SPANS).astype(jnp.int32)
    return dict(query=query, key=key, value=value, span_order=span_order)


masked_score = -1.0e30


def reference(query, key, value, span_order):
    group = QHEADS // KVHEADS
    groups = SEQ // GROUP_ROWS
    offsets = jnp.arange(TOK_DEV, dtype=jnp.int32)
    positions = (span_order.astype(jnp.int32)[:, None] * TOK_DEV + offsets[None, :]).astype(jnp.int32)
    queries = query.reshape(SPANS, TOK_DEV, KVHEADS, group, HEAD_DIM)
    keys = key.reshape(groups, GROUP_ROWS, KVHEADS, HEAD_DIM)
    values = value.reshape(groups, GROUP_ROWS, KVHEADS, HEAD_DIM)
    key_places = positions.reshape(groups, GROUP_ROWS)

    def one_span(inputs):
        span_queries, span_places = inputs
        span_queries = span_queries.astype(jnp.float32)

        def live_group(group_in):
            group_keys, group_values, group_places = group_in
            scores = jnp.einsum("nkgd,skd->nkgs", span_queries, group_keys.astype(jnp.float32)) * (HEAD_DIM ** -0.5)
            visible = group_places[None, None, None, :] <= span_places[:, None, None, None]
            scores = jnp.where(visible, scores, masked_score)
            top = jnp.max(scores, axis=-1)
            raised = jnp.exp(scores - top[..., None])
            total = jnp.sum(raised, axis=-1)
            weights = lax.optimization_barrier(raised.astype(jnp.bfloat16)).astype(jnp.float32)
            summed = jnp.einsum("nkgs,skd->nkgd", weights, group_values.astype(jnp.float32))
            floor = jnp.maximum(total, 1.0)
            partial_value = lax.optimization_barrier((summed / floor[..., None]).astype(jnp.bfloat16)).astype(jnp.float32)
            return partial_value, top + jnp.log(floor)

        def dead_group(group_in):
            partial_value = jnp.zeros((TOK_DEV, KVHEADS, group, HEAD_DIM), span_queries.dtype)
            log_sum = jnp.full((TOK_DEV, KVHEADS, group), masked_score, span_queries.dtype)
            return partial_value, log_sum

        def one_group(group_in):
            group_places = group_in[2]
            alive = jnp.min(group_places) <= jnp.max(span_places)
            return lax.cond(alive, live_group, dead_group, group_in)

        partials, log_sums = lax.map(one_group, (keys, values, key_places))
        highest = jnp.max(log_sums, axis=0)
        combined = highest + jnp.log(jnp.sum(jnp.exp(log_sums - highest), axis=0))
        scale_each = jnp.exp(log_sums - combined)
        merged = jnp.sum(scale_each[..., None] * partials, axis=0)
        return merged.astype(jnp.bfloat16)

    result = lax.map(one_span, (queries, positions))
    return result.reshape(SEQ, QHEADS * HEAD_DIM)
```

```python
import functools
import math

import jax
import jax.numpy as jnp
from jax import lax
from jax.experimental import pallas as pl
from jax.experimental.pallas import tpu as pltpu
from jax.sharding import PartitionSpec as P

HEAD_DIM = 128
QHEADS = 32
KVHEADS = 4
GROUP = QHEADS // KVHEADS
masked_score = -1e30
MESH = pl.DeviceIdType.MESH
VMEM_LIMIT = 60 * 1024 * 1024


def device(row, col):
    return {"row": row, "col": col}


def spread_kernel(rows, cols, key_ref, value_ref, out_ref, held, own_sem, plane_send, plane_recv,
                  col_send, col_recv, side_send, side_recv, out_sem):
    share = rows // KVHEADS
    row, col = lax.axis_index("row"), lax.axis_index("col")
    head, lane = row // share, row % share
    peers = []
    for step in range(1, KVHEADS):
        peers.append((lax.rem(head + step, KVHEADS) * share + lane, col))
    for step in range(1, cols):
        peers.append((row, lax.rem(col + step, cols)))
    for step in range(1, share):
        peers.append((head * share + lax.rem(lane + step, share), col))
    barrier = pltpu.get_barrier_semaphore()
    for peer in peers:
        pl.semaphore_signal(barrier, inc=1, device_id=device(*peer), device_id_type=MESH)
    pl.semaphore_wait(barrier, len(peers))

    sent = []
    plane = []
    for step in range(1, KVHEADS):
        other = lax.rem(head + step, KVHEADS)
        columns = pl.ds(pl.multiple_of(other * HEAD_DIM, HEAD_DIM), HEAD_DIM)
        for kind, ref in enumerate((key_ref, value_ref)):
            copy = pltpu.make_async_remote_copy(
                src_ref=ref.at[:, columns],
                dst_ref=held.at[col, lane, head, kind],
                send_sem=plane_send.at[step - 1, kind],
                recv_sem=plane_recv.at[step - 1, kind],
                device_id=device(other * share + lane, col),
                device_id_type=MESH,
            )
            copy.start()
            plane.append(copy)
    columns = pl.ds(pl.multiple_of(head * HEAD_DIM, HEAD_DIM), HEAD_DIM)
    own = []
    for kind, ref in enumerate((key_ref, value_ref)):
        copy = pltpu.make_async_copy(ref.at[:, columns], held.at[col, lane, head, kind], own_sem.at[kind])
        copy.start()
        own.append(copy)
    for copy in own:
        copy.wait()
    for copy in plane:
        copy.wait_recv()
    sent += plane
    along = []
    for step in range(1, cols):
        copy = pltpu.make_async_remote_copy(
            src_ref=held.at[col, lane],
            dst_ref=held.at[col, lane],
            send_sem=col_send.at[step - 1],
            recv_sem=col_recv.at[step - 1],
            device_id=device(row, lax.rem(col + step, cols)),
            device_id_type=MESH,
        )
        copy.start()
        along.append(copy)
    sent += along
    stores = []
    side = []
    for step in range(cols):
        source = lax.rem(col - step + cols, cols)
        if step:
            along[step - 1].wait_recv()
        for other in range(1, share):
            copy = pltpu.make_async_remote_copy(
                src_ref=held.at[source, lane],
                dst_ref=held.at[source, lane],
                send_sem=side_send.at[step, other - 1],
                recv_sem=side_recv.at[step, other - 1],
                device_id=device(head * share + lax.rem(lane + other, share), col),
                device_id_type=MESH,
            )
            copy.start()
            side.append((copy, source, other, step))
        store = pltpu.make_async_copy(held.at[source, lane], out_ref.at[source, lane], out_sem.at[step, 0])
        store.start()
        stores.append(store)
    for copy, source, other, step in side:
        copy.wait_recv()
        there = lax.rem(lane - other + share, share)
        store = pltpu.make_async_copy(held.at[source, there], out_ref.at[source, there], out_sem.at[step, other])
        store.start()
        stores.append(store)
        sent.append(copy)
    for copy in sent:
        copy.wait_send()
    for store in stores:
        store.wait()


def spread(key, value, rows, cols):
    share = rows // KVHEADS
    tokens = key.shape[0]
    shape = (cols, share, KVHEADS, 2, tokens, HEAD_DIM)
    dma = pltpu.SemaphoreType.DMA
    return pl.pallas_call(
        functools.partial(spread_kernel, rows, cols),
        out_shape=jax.ShapeDtypeStruct(shape, key.dtype),
        in_specs=[pl.BlockSpec(memory_space=pltpu.VMEM)] * 2,
        out_specs=pl.BlockSpec(memory_space=pl.ANY),
        scratch_shapes=[
            pltpu.VMEM(shape, key.dtype),
            dma((2,)),
            dma((KVHEADS - 1, 2)),
            dma((KVHEADS - 1, 2)),
            dma((cols - 1,)),
            dma((cols - 1,)),
            dma((cols, share - 1)),
            dma((cols, share - 1)),
            dma((cols, share)),
        ],
        compiler_params=pltpu.CompilerParams(
            collective_id=0, has_side_effects=True, vmem_limit_bytes=VMEM_LIMIT
        ),
        name="spread",
    )(key, value)


def attend_kernel(cols, share, chunk_spans, order_ref, place_ref, query_ref, held_ref, out_ref,
                  keys, values, queries, best, total):
    tokens = query_ref.shape[1]
    heads = query_ref.shape[2] // HEAD_DIM
    count = heads * tokens
    spans = order_ref.shape[0]
    step = pl.program_id(0)
    width = chunk_spans * tokens

    @pl.when(step == 0)
    def _():
        values[:, HEAD_DIM:] = jnp.ones((values.shape[0], HEAD_DIM), values.dtype)

        def place(span, carry):
            row, col = span // cols, span % cols
            spot = pl.ds(pl.multiple_of(order_ref[span] * tokens, tokens), tokens)
            block = held_ref[col, row % share, row // share, 0]
            keys[spot, :HEAD_DIM] = block
            keys[spot, HEAD_DIM:] = block
            values[spot, :HEAD_DIM] = held_ref[col, row % share, row // share, 1]
            return carry

        lax.fori_loop(0, spans, place, 0)

    scale = math.log2(math.e) / math.sqrt(HEAD_DIM)
    for head in range(heads):
        part = query_ref[0, :, head * HEAD_DIM : (head + 1) * HEAD_DIM].astype(jnp.float32) * scale
        high = part.astype(jnp.bfloat16)
        low = (part - high.astype(jnp.float32)).astype(jnp.bfloat16)
        queries[head * tokens : (head + 1) * tokens, :HEAD_DIM] = high
        queries[head * tokens : (head + 1) * tokens, HEAD_DIM:] = low

    mine = order_ref[step * cols + place_ref[1]]
    last = mine // chunk_spans
    strip = 2 * tokens if heads % 2 == 0 else tokens

    def chunk(index, first):
        spot = pl.ds(pl.multiple_of(index * width, width), width)
        for start in range(0, count, strip):
            lines = slice(start, start + strip)
            scores = lax.dot_general(
                queries[lines, :], keys[spot, :], (((1,), (1,)), ((), ())), preferred_element_type=jnp.float32
            )
            if first:
                below = lax.broadcasted_iota(jnp.int32, scores.shape, 0) % tokens
                across = lax.broadcasted_iota(jnp.int32, scores.shape, 1)
                scores = jnp.where(across <= below + (mine % chunk_spans) * tokens, scores, masked_score)
                newest = jnp.max(scores, axis=1, keepdims=True)
            else:
                before = best[lines, :1]
                newest = jnp.maximum(before, jnp.max(scores, axis=1, keepdims=True))
            raised = jnp.exp2(scores - newest).astype(jnp.bfloat16)
            update = jnp.dot(raised, values[spot, :], preferred_element_type=jnp.float32)
            if first:
                total[lines, :] = update
            else:
                total[lines, :] = total[lines, :] * jnp.exp2(before - newest) + update
            best[lines, :] = jnp.broadcast_to(newest, (strip, HEAD_DIM))

    chunk(last, True)

    def body(index, carry):
        chunk(index, False)
        return carry

    lax.fori_loop(0, last, body, 0)
    for head in range(heads):
        lines = slice(head * tokens, (head + 1) * tokens)
        out_ref[0, :, head * HEAD_DIM : (head + 1) * HEAD_DIM] = (
            total[lines, :HEAD_DIM] / total[lines, HEAD_DIM:]
        ).astype(out_ref.dtype)


def attend(query, held, span_order, rows, cols):
    share = rows // KVHEADS
    tokens = query.shape[1]
    width = query.shape[2] // rows
    spans = span_order.shape[0]
    sequence = spans * tokens
    count = width // HEAD_DIM * tokens
    chunk_spans = 4
    place = jnp.stack([lax.axis_index("row"), lax.axis_index("col")]).astype(jnp.int32)
    return pl.pallas_call(
        functools.partial(attend_kernel, cols, share, chunk_spans),
        out_shape=jax.ShapeDtypeStruct((rows, tokens, width), query.dtype),
        grid_spec=pltpu.PrefetchScalarGridSpec(
            num_scalar_prefetch=2,
            grid=(rows,),
            in_specs=[
                pl.BlockSpec((1, tokens, width), lambda step, order, place: (step, 0, place[0])),
                pl.BlockSpec(held.shape, lambda step, order, place: (0,) * held.ndim),
            ],
            out_specs=pl.BlockSpec((1, tokens, width), lambda step, order, place: (step, 0, 0)),
            scratch_shapes=[
                pltpu.VMEM((sequence, 2 * HEAD_DIM), jnp.bfloat16),
                pltpu.VMEM((sequence, 2 * HEAD_DIM), jnp.bfloat16),
                pltpu.VMEM((count, 2 * HEAD_DIM), jnp.bfloat16),
                pltpu.VMEM((count, HEAD_DIM), jnp.float32),
                pltpu.VMEM((count, 2 * HEAD_DIM), jnp.float32),
            ],
        ),
        compiler_params=pltpu.CompilerParams(
            dimension_semantics=("arbitrary",), vmem_limit_bytes=VMEM_LIMIT
        ),
        name="attend",
    )(span_order, place, query, held)


def deliver_kernel(rows, part_ref, out_ref, own_sem, send_sem, recv_sem):
    row, col = lax.axis_index("row"), lax.axis_index("col")
    width = part_ref.shape[2]
    barrier = pltpu.get_barrier_semaphore()
    for step in range(1, rows):
        pl.semaphore_signal(
            barrier, inc=1, device_id=device(lax.rem(row + step, rows), col), device_id_type=MESH
        )
    pl.semaphore_wait(barrier, rows - 1)
    columns = pl.ds(pl.multiple_of(row * width, width), width)
    copies = []
    for step in range(1, rows):
        target = lax.rem(row + step, rows)
        copy = pltpu.make_async_remote_copy(
            src_ref=part_ref.at[target],
            dst_ref=out_ref.at[:, columns],
            send_sem=send_sem.at[step - 1],
            recv_sem=recv_sem.at[step - 1],
            device_id=device(target, col),
            device_id_type=MESH,
        )
        copy.start()
        copies.append(copy)
    own = pltpu.make_async_copy(part_ref.at[row], out_ref.at[:, columns], own_sem)
    own.start()
    own.wait()
    for copy in copies:
        copy.wait()


def deliver(parts):
    rows, tokens, width = parts.shape
    dma = pltpu.SemaphoreType.DMA
    return pl.pallas_call(
        functools.partial(deliver_kernel, rows),
        out_shape=jax.ShapeDtypeStruct((tokens, rows * width), parts.dtype),
        in_specs=[pl.BlockSpec(memory_space=pltpu.VMEM)],
        out_specs=pl.BlockSpec(memory_space=pl.ANY),
        scratch_shapes=[dma(()), dma((rows - 1,)), dma((rows - 1,))],
        compiler_params=pltpu.CompilerParams(
            collective_id=1, has_side_effects=True, vmem_limit_bytes=VMEM_LIMIT
        ),
        name="deliver",
    )(parts)


def shards(query, key, value, span_order):
    rows = lax.axis_size("row")
    cols = lax.axis_size("col")
    held = spread(key, value, rows, cols)
    parts = attend(query, held, span_order, rows, cols)
    return deliver(parts)


def solution(mesh):
    placed = (P(None, "col", None), P(("row", "col"), None), P(("row", "col"), None), P())
    return jax.shard_map(
        shards, mesh=mesh, in_specs=placed, out_specs=P(("row", "col"), None), check_vma=False
    )
```

```python
import functools
import math

import jax
import jax.numpy as jnp
from jax import lax
from jax.experimental import pallas as pl
from jax.experimental.pallas import tpu as pltpu
from jax.sharding import PartitionSpec as P

HEAD_DIM = 128
QHEADS = 32
KVHEADS = 4
GROUP = QHEADS // KVHEADS
masked_score = -1e30
MESH = pl.DeviceIdType.MESH
VMEM_LIMIT = 60 * 1024 * 1024


def device(row, col):
    return {"row": row, "col": col}


def spread_kernel(rows, cols, key_ref, value_ref, out_ref, held, own_sem, plane_send, plane_recv,
                  col_send, col_recv, side_send, side_recv, out_sem):
    share = rows // KVHEADS
    row, col = lax.axis_index("row"), lax.axis_index("col")
    head, lane = row // share, row % share
    barrier = pltpu.get_barrier_semaphore()
    peers = [(lax.rem(head + step, KVHEADS) * share + lane, col) for step in range(1, KVHEADS)]
    peers += [(head * share + lax.rem(lane + step, share), col) for step in range(1, share)]
    for peer in peers:
        pl.semaphore_signal(barrier, inc=1, device_id=device(*peer), device_id_type=MESH)
    ways = (1, -1)
    for way in ways:
        beside = jnp.logical_and(col + way >= 0, col + way < cols)

        @pl.when(beside)
        def _(way=way):
            pl.semaphore_signal(barrier, inc=1, device_id=device(row, col + way), device_id_type=MESH)

    ends = jnp.where(col == 0, 1, 0) + jnp.where(col == cols - 1, 1, 0)
    pl.semaphore_wait(barrier, len(peers) + len(ways) - ends)

    plane = []
    for step in range(1, KVHEADS):
        other = lax.rem(head + step, KVHEADS)
        columns = pl.ds(pl.multiple_of(other * HEAD_DIM, HEAD_DIM), HEAD_DIM)
        for kind, ref in enumerate((key_ref, value_ref)):
            copy = pltpu.make_async_remote_copy(
                src_ref=ref.at[:, columns],
                dst_ref=held.at[col, lane, head, kind],
                send_sem=plane_send.at[step - 1, kind],
                recv_sem=plane_recv.at[step - 1, kind],
                device_id=device(other * share + lane, col),
                device_id_type=MESH,
            )
            copy.start()
            plane.append(copy)
    columns = pl.ds(pl.multiple_of(head * HEAD_DIM, HEAD_DIM), HEAD_DIM)
    own = []
    for kind, ref in enumerate((key_ref, value_ref)):
        copy = pltpu.make_async_copy(ref.at[:, columns], held.at[col, lane, head, kind], own_sem.at[kind])
        copy.start()
        own.append(copy)
    for copy in own:
        copy.wait()

    def slot_of(piece):
        return lax.rem(head - piece + KVHEADS, KVHEADS)

    def source_of(step, way):
        return col - way * step

    def way_index(way):
        return ways.index(way)

    def held_here(step, way):
        source = source_of(step, way)
        return jnp.logical_and(source >= 0, source < cols)

    def passes_on(step, way):
        target = col + way
        return jnp.logical_and(held_here(step, way), jnp.logical_and(target >= 0, target < cols))

    def on_copy(step, way, piece):
        spot = held.at[source_of(step, way), lane, slot_of(piece)]
        return pltpu.make_async_remote_copy(
            src_ref=spot,
            dst_ref=spot,
            send_sem=col_send.at[step, way_index(way), piece],
            recv_sem=col_recv.at[step, way_index(way), piece],
            device_id=device(row, col + way),
            device_id_type=MESH,
        )

    def in_copy(step, way, piece):
        spot = held.at[source_of(step + 1, way), lane, slot_of(piece)]
        return pltpu.make_async_remote_copy(
            src_ref=spot,
            dst_ref=spot,
            send_sem=col_send.at[step, way_index(way), piece],
            recv_sem=col_recv.at[step, way_index(way), piece],
            device_id=device(row, col - way),
            device_id_type=MESH,
        )

    def side_copy(step, way, piece, other, arriving):
        there = lax.rem(lane - other + share, share) if arriving else lane
        spot = held.at[source_of(step, way), there, slot_of(piece)]
        return pltpu.make_async_remote_copy(
            src_ref=spot,
            dst_ref=spot,
            send_sem=side_send.at[step, way_index(way), piece, other - 1],
            recv_sem=side_recv.at[step, way_index(way), piece, other - 1],
            device_id=device(head * share + lax.rem(lane + other, share), col),
            device_id_type=MESH,
        )

    def out_copy(step, way, other):
        there = lax.rem(lane - other + share, share)
        source = source_of(step, way)
        return pltpu.make_async_copy(
            held.at[source, there], out_ref.at[source, there], out_sem.at[step, way_index(way), other]
        )

    def store(step):
        for way in ways if step else (1,):
            @pl.when(held_here(step, way))
            def _(way=way):
                for other in range(share):
                    if other:
                        for piece in range(KVHEADS):
                            side_copy(step, way, piece, other, True).wait_recv()
                    out_copy(step, way, other).start()

    for step in range(cols):
        for piece in range(KVHEADS):
            if step == 0 and piece:
                for copy in plane[2 * (piece - 1) : 2 * piece]:
                    copy.wait_recv()
            for way in ways:
                if step:
                    @pl.when(held_here(step, way))
                    def _(way=way):
                        in_copy(step - 1, way, piece).wait_recv()

                if step < cols - 1:
                    @pl.when(passes_on(step, way))
                    def _(way=way):
                        on_copy(step, way, piece).start()

                if step or way == 1:
                    @pl.when(held_here(step, way))
                    def _(way=way):
                        for other in range(1, share):
                            side_copy(step, way, piece, other, False).start()

        if step:
            store(step - 1)
    store(cols - 1)
    for copy in plane:
        copy.wait_send()
    for step in range(cols):
        for way in ways:
            if step < cols - 1:
                @pl.when(passes_on(step, way))
                def _(way=way):
                    for piece in range(KVHEADS):
                        on_copy(step, way, piece).wait_send()

            if step or way == 1:
                @pl.when(held_here(step, way))
                def _(way=way):
                    for other in range(share):
                        if other:
                            for piece in range(KVHEADS):
                                side_copy(step, way, piece, other, False).wait_send()
                        out_copy(step, way, other).wait()


def spread(key, value, rows, cols):
    share = rows // KVHEADS
    tokens = key.shape[0]
    shape = (cols, share, KVHEADS, 2, tokens, HEAD_DIM)
    dma = pltpu.SemaphoreType.DMA
    return pl.pallas_call(
        functools.partial(spread_kernel, rows, cols),
        out_shape=jax.ShapeDtypeStruct(shape, key.dtype),
        in_specs=[pl.BlockSpec(memory_space=pltpu.VMEM)] * 2,
        out_specs=pl.BlockSpec(memory_space=pl.ANY),
        scratch_shapes=[
            pltpu.VMEM(shape, key.dtype),
            dma((2,)),
            dma((KVHEADS - 1, 2)),
            dma((KVHEADS - 1, 2)),
            dma((cols - 1, 2, KVHEADS)),
            dma((cols - 1, 2, KVHEADS)),
            dma((cols, 2, KVHEADS, share - 1)),
            dma((cols, 2, KVHEADS, share - 1)),
            dma((cols, 2, share)),
        ],
        compiler_params=pltpu.CompilerParams(
            collective_id=0, has_side_effects=True, vmem_limit_bytes=VMEM_LIMIT
        ),
        name="spread",
    )(key, value)


def attend_kernel(cols, share, chunk_spans, order_ref, place_ref, query_ref, held_ref, out_ref,
                  keys, values, queries, best, total, ahead):
    tokens = query_ref.shape[1]
    heads = query_ref.shape[2] // HEAD_DIM
    count = heads * tokens
    spans = order_ref.shape[0]
    step = pl.program_id(0)
    width = chunk_spans * tokens

    @pl.when(step == 0)
    def _():
        values[:, HEAD_DIM:] = jnp.ones((values.shape[0], HEAD_DIM), values.dtype)

        def place(span, carry):
            row, col = span // cols, span % cols
            spot = pl.ds(pl.multiple_of(order_ref[span] * tokens, tokens), tokens)
            block = held_ref[col, row % share, row // share, 0]
            turned = block.astype(jnp.float32).T.astype(block.dtype)
            keys[:HEAD_DIM, spot] = turned
            keys[HEAD_DIM:, spot] = turned
            values[spot, :HEAD_DIM] = held_ref[col, row % share, row // share, 1]
            return carry

        lax.fori_loop(0, spans, place, 0)

    scale = math.log2(math.e) / math.sqrt(HEAD_DIM)
    for head in range(heads):
        part = query_ref[0, :, head * HEAD_DIM : (head + 1) * HEAD_DIM].astype(jnp.float32) * scale
        high = part.astype(jnp.bfloat16)
        low = (part - high.astype(jnp.float32)).astype(jnp.bfloat16)
        queries[head * tokens : (head + 1) * tokens, :HEAD_DIM] = high
        queries[head * tokens : (head + 1) * tokens, HEAD_DIM:] = low

    mine = order_ref[step * cols + place_ref[1]]
    last = mine // chunk_spans

    def spot(index):
        return pl.ds(pl.multiple_of(index * width, width), width)

    def score(index):
        return jnp.dot(queries[...], keys[:, spot(index)], preferred_element_type=jnp.float32)

    def top_of(scores):
        return jnp.broadcast_to(jnp.max(scores, axis=1, keepdims=True), (count, HEAD_DIM))

    def weigh(scores, newest, index):
        raised = jnp.exp2(scores - jnp.concatenate([newest] * chunk_spans, axis=1)).astype(jnp.bfloat16)
        return jnp.dot(raised, values[spot(index), :], preferred_element_type=jnp.float32)

    scores = score(last)
    below = lax.broadcasted_iota(jnp.int32, scores.shape, 0) % tokens
    across = lax.broadcasted_iota(jnp.int32, scores.shape, 1)
    scores = jnp.where(across <= below + (mine % chunk_spans) * tokens, scores, masked_score)
    newest = top_of(scores)
    ahead[...] = score(0)
    total[...] = weigh(scores, newest, last)
    best[...] = newest

    def body(index, carry):
        scores = ahead[...]
        before = best[...]
        newest = jnp.maximum(before, top_of(scores))
        shrink = jnp.exp2(before - newest)
        ahead[...] = score(jnp.minimum(index + 1, last))
        update = weigh(scores, newest, index)
        total[...] = total[...] * jnp.concatenate([shrink] * 2, axis=1) + update
        best[...] = newest
        return carry

    lax.fori_loop(0, last, body, 0)
    for head in range(heads):
        lines = slice(head * tokens, (head + 1) * tokens)
        out_ref[0, :, head * HEAD_DIM : (head + 1) * HEAD_DIM] = (
            total[lines, :HEAD_DIM] / total[lines, HEAD_DIM:]
        ).astype(out_ref.dtype)


def attend(query, held, span_order, rows, cols):
    share = rows // KVHEADS
    tokens = query.shape[1]
    width = query.shape[2] // rows
    spans = span_order.shape[0]
    sequence = spans * tokens
    count = width // HEAD_DIM * tokens
    chunk_spans = 4
    place = jnp.stack([lax.axis_index("row"), lax.axis_index("col")]).astype(jnp.int32)
    return pl.pallas_call(
        functools.partial(attend_kernel, cols, share, chunk_spans),
        out_shape=jax.ShapeDtypeStruct((rows, tokens, width), query.dtype),
        grid_spec=pltpu.PrefetchScalarGridSpec(
            num_scalar_prefetch=2,
            grid=(rows,),
            in_specs=[
                pl.BlockSpec((1, tokens, width), lambda step, order, place: (step, 0, place[0])),
                pl.BlockSpec(held.shape, lambda step, order, place: (0,) * held.ndim),
            ],
            out_specs=pl.BlockSpec((1, tokens, width), lambda step, order, place: (step, 0, 0)),
            scratch_shapes=[
                pltpu.VMEM((2 * HEAD_DIM, sequence), jnp.bfloat16),
                pltpu.VMEM((sequence, 2 * HEAD_DIM), jnp.bfloat16),
                pltpu.VMEM((count, 2 * HEAD_DIM), jnp.bfloat16),
                pltpu.VMEM((count, HEAD_DIM), jnp.float32),
                pltpu.VMEM((count, 2 * HEAD_DIM), jnp.float32),
                pltpu.VMEM((count, chunk_spans * tokens), jnp.float32),
            ],
        ),
        compiler_params=pltpu.CompilerParams(
            dimension_semantics=("arbitrary",), vmem_limit_bytes=VMEM_LIMIT
        ),
        name="attend",
    )(span_order, place, query, held)


def deliver_kernel(rows, part_ref, out_ref, own_sem, send_sem, recv_sem):
    row, col = lax.axis_index("row"), lax.axis_index("col")
    width = part_ref.shape[2]
    barrier = pltpu.get_barrier_semaphore()
    for step in range(1, rows):
        pl.semaphore_signal(
            barrier, inc=1, device_id=device(lax.rem(row + step, rows), col), device_id_type=MESH
        )
    pl.semaphore_wait(barrier, rows - 1)
    columns = pl.ds(pl.multiple_of(row * width, width), width)
    copies = []
    for step in range(1, rows):
        target = lax.rem(row + step, rows)
        copy = pltpu.make_async_remote_copy(
            src_ref=part_ref.at[target],
            dst_ref=out_ref.at[:, columns],
            send_sem=send_sem.at[step - 1],
            recv_sem=recv_sem.at[step - 1],
            device_id=device(target, col),
            device_id_type=MESH,
        )
        copy.start()
        copies.append(copy)
    own = pltpu.make_async_copy(part_ref.at[row], out_ref.at[:, columns], own_sem)
    own.start()
    own.wait()
    for copy in copies:
        copy.wait()


def deliver(parts):
    rows, tokens, width = parts.shape
    dma = pltpu.SemaphoreType.DMA
    return pl.pallas_call(
        functools.partial(deliver_kernel, rows),
        out_shape=jax.ShapeDtypeStruct((tokens, rows * width), parts.dtype),
        in_specs=[pl.BlockSpec(memory_space=pltpu.VMEM)],
        out_specs=pl.BlockSpec(memory_space=pl.ANY),
        scratch_shapes=[dma(()), dma((rows - 1,)), dma((rows - 1,))],
        compiler_params=pltpu.CompilerParams(
            collective_id=1, has_side_effects=True, vmem_limit_bytes=VMEM_LIMIT
        ),
        name="deliver",
    )(parts)


def shards(query, key, value, span_order):
    rows = lax.axis_size("row")
    cols = lax.axis_size("col")
    held = spread(key, value, rows, cols)
    parts = attend(query, held, span_order, rows, cols)
    return deliver(parts)


def solution(mesh):
    placed = (P(None, "col", None), P(("row", "col"), None), P(("row", "col"), None), P())
    return jax.shard_map(
        shards, mesh=mesh, in_specs=placed, out_specs=P(("row", "col"), None), check_vma=False
    )
```

```python
import functools
import math

import jax
import jax.numpy as jnp
from jax import lax
from jax.experimental import pallas as pl
from jax.experimental.pallas import tpu as pltpu
from jax.sharding import PartitionSpec as P

HEAD_DIM = 128
QHEADS = 32
KVHEADS = 4
GROUP = QHEADS // KVHEADS
masked_score = -1e30
MESH = pl.DeviceIdType.MESH
VMEM_LIMIT = 60 * 1024 * 1024


def device(row, col):
    return {"row": row, "col": col}


def spread_kernel(rows, cols, key_ref, value_ref, out_ref, held, own_sem, plane_send, plane_recv,
                  col_send, col_recv, side_send, side_recv, out_sem):
    share = rows // KVHEADS
    row, col = lax.axis_index("row"), lax.axis_index("col")
    head, lane = row // share, row % share
    barrier = pltpu.get_barrier_semaphore()
    peers = [(lax.rem(head + step, KVHEADS) * share + lane, col) for step in range(1, KVHEADS)]
    peers += [(head * share + lax.rem(lane + step, share), col) for step in range(1, share)]
    for peer in peers:
        pl.semaphore_signal(barrier, inc=1, device_id=device(*peer), device_id_type=MESH)
    ways = (1, -1)
    for way in ways:
        beside = jnp.logical_and(col + way >= 0, col + way < cols)

        @pl.when(beside)
        def _(way=way):
            pl.semaphore_signal(barrier, inc=1, device_id=device(row, col + way), device_id_type=MESH)

    ends = jnp.where(col == 0, 1, 0) + jnp.where(col == cols - 1, 1, 0)
    pl.semaphore_wait(barrier, len(peers) + len(ways) - ends)

    plane = []
    for step in range(1, KVHEADS):
        other = lax.rem(head + step, KVHEADS)
        columns = pl.ds(pl.multiple_of(other * HEAD_DIM, HEAD_DIM), HEAD_DIM)
        for kind, ref in enumerate((key_ref, value_ref)):
            copy = pltpu.make_async_remote_copy(
                src_ref=ref.at[:, columns],
                dst_ref=held.at[col, lane, head, kind],
                send_sem=plane_send.at[step - 1, kind],
                recv_sem=plane_recv.at[step - 1, kind],
                device_id=device(other * share + lane, col),
                device_id_type=MESH,
            )
            copy.start()
            plane.append(copy)
    columns = pl.ds(pl.multiple_of(head * HEAD_DIM, HEAD_DIM), HEAD_DIM)
    own = []
    for kind, ref in enumerate((key_ref, value_ref)):
        copy = pltpu.make_async_copy(ref.at[:, columns], held.at[col, lane, head, kind], own_sem.at[kind])
        copy.start()
        own.append(copy)
    for copy in own:
        copy.wait()

    def slot_of(piece):
        return lax.rem(head - piece + KVHEADS, KVHEADS)

    def source_of(step, way):
        return col - way * step

    def way_index(way):
        return ways.index(way)

    def held_here(step, way):
        source = source_of(step, way)
        return jnp.logical_and(source >= 0, source < cols)

    def passes_on(step, way):
        target = col + way
        return jnp.logical_and(held_here(step, way), jnp.logical_and(target >= 0, target < cols))

    def on_copy(step, way, piece):
        spot = held.at[source_of(step, way), lane, slot_of(piece)]
        return pltpu.make_async_remote_copy(
            src_ref=spot,
            dst_ref=spot,
            send_sem=col_send.at[step, way_index(way), piece],
            recv_sem=col_recv.at[step, way_index(way), piece],
            device_id=device(row, col + way),
            device_id_type=MESH,
        )

    def in_copy(step, way, piece):
        spot = held.at[source_of(step + 1, way), lane, slot_of(piece)]
        return pltpu.make_async_remote_copy(
            src_ref=spot,
            dst_ref=spot,
            send_sem=col_send.at[step, way_index(way), piece],
            recv_sem=col_recv.at[step, way_index(way), piece],
            device_id=device(row, col - way),
            device_id_type=MESH,
        )

    def side_copy(step, way, piece, other, arriving):
        there = lax.rem(lane - other + share, share) if arriving else lane
        spot = held.at[source_of(step, way), there, slot_of(piece)]
        return pltpu.make_async_remote_copy(
            src_ref=spot,
            dst_ref=spot,
            send_sem=side_send.at[step, way_index(way), piece, other - 1],
            recv_sem=side_recv.at[step, way_index(way), piece, other - 1],
            device_id=device(head * share + lax.rem(lane + other, share), col),
            device_id_type=MESH,
        )

    def out_copy(step, way, other):
        there = lax.rem(lane - other + share, share)
        source = source_of(step, way)
        return pltpu.make_async_copy(
            held.at[source, there], out_ref.at[source, there], out_sem.at[step, way_index(way), other]
        )

    def store(step):
        for way in ways if step else (1,):
            @pl.when(held_here(step, way))
            def _(way=way):
                for other in range(share):
                    if other:
                        for piece in range(KVHEADS):
                            side_copy(step, way, piece, other, True).wait_recv()
                    out_copy(step, way, other).start()

    for step in range(cols):
        for piece in range(KVHEADS):
            if step == 0 and piece:
                for copy in plane[2 * (piece - 1) : 2 * piece]:
                    copy.wait_recv()
            for way in ways:
                if step:
                    @pl.when(held_here(step, way))
                    def _(way=way):
                        in_copy(step - 1, way, piece).wait_recv()

                if step < cols - 1:
                    @pl.when(passes_on(step, way))
                    def _(way=way):
                        on_copy(step, way, piece).start()

                if step or way == 1:
                    @pl.when(held_here(step, way))
                    def _(way=way):
                        for other in range(1, share):
                            side_copy(step, way, piece, other, False).start()

        if step:
            store(step - 1)
    store(cols - 1)
    for copy in plane:
        copy.wait_send()
    for step in range(cols):
        for way in ways:
            if step < cols - 1:
                @pl.when(passes_on(step, way))
                def _(way=way):
                    for piece in range(KVHEADS):
                        on_copy(step, way, piece).wait_send()

            if step or way == 1:
                @pl.when(held_here(step, way))
                def _(way=way):
                    for other in range(share):
                        if other:
                            for piece in range(KVHEADS):
                                side_copy(step, way, piece, other, False).wait_send()
                        out_copy(step, way, other).wait()


def spread(key, value, rows, cols):
    share = rows // KVHEADS
    tokens = key.shape[0]
    shape = (cols, share, KVHEADS, 2, tokens, HEAD_DIM)
    dma = pltpu.SemaphoreType.DMA
    return pl.pallas_call(
        functools.partial(spread_kernel, rows, cols),
        out_shape=jax.ShapeDtypeStruct(shape, key.dtype),
        in_specs=[pl.BlockSpec(memory_space=pltpu.VMEM)] * 2,
        out_specs=pl.BlockSpec(memory_space=pl.ANY),
        scratch_shapes=[
            pltpu.VMEM(shape, key.dtype),
            dma((2,)),
            dma((KVHEADS - 1, 2)),
            dma((KVHEADS - 1, 2)),
            dma((cols - 1, 2, KVHEADS)),
            dma((cols - 1, 2, KVHEADS)),
            dma((cols, 2, KVHEADS, share - 1)),
            dma((cols, 2, KVHEADS, share - 1)),
            dma((cols, 2, share)),
        ],
        compiler_params=pltpu.CompilerParams(
            collective_id=0, has_side_effects=True, vmem_limit_bytes=VMEM_LIMIT
        ),
        name="spread",
    )(key, value)


def attend_kernel(cols, share, chunk_spans, order_ref, query_ref, held_ref, out_ref,
                  keys, values, queries, best, total, ahead):
    tokens = query_ref.shape[1]
    heads = query_ref.shape[2] // HEAD_DIM
    count = heads * tokens
    spans = order_ref.shape[0]
    step = pl.program_id(0)
    width = chunk_spans * tokens

    @pl.when(step == 0)
    def _():
        values[:, HEAD_DIM:] = jnp.ones((values.shape[0], HEAD_DIM), values.dtype)

        def place(span, carry):
            row, col = span // cols, span % cols
            spot = pl.ds(pl.multiple_of(order_ref[span] * tokens, tokens), tokens)
            block = held_ref[col, row % share, row // share, 0]
            turned = block.T
            keys[:HEAD_DIM, spot] = turned
            keys[HEAD_DIM:, spot] = turned
            values[spot, :HEAD_DIM] = held_ref[col, row % share, row // share, 1]
            return carry

        lax.fori_loop(0, spans, place, 0, unroll=8)

    scale = math.log2(math.e) / math.sqrt(HEAD_DIM)
    for head in range(heads):
        part = query_ref[0, :, head * HEAD_DIM : (head + 1) * HEAD_DIM].astype(jnp.float32) * scale
        high = part.astype(jnp.bfloat16)
        low = (part - high.astype(jnp.float32)).astype(jnp.bfloat16)
        queries[head * tokens : (head + 1) * tokens, :HEAD_DIM] = high
        queries[head * tokens : (head + 1) * tokens, HEAD_DIM:] = low

    mine = order_ref[step * cols + lax.axis_index("col")]
    last = mine // chunk_spans

    def spot(index):
        return pl.ds(pl.multiple_of(index * width, width), width)

    def score(index):
        return jnp.dot(queries[...], keys[:, spot(index)], preferred_element_type=jnp.float32)

    def top_of(scores):
        return jnp.broadcast_to(jnp.max(scores, axis=1, keepdims=True), (count, HEAD_DIM))

    def weigh(scores, newest, index):
        raised = jnp.exp2(scores - jnp.concatenate([newest] * chunk_spans, axis=1)).astype(jnp.bfloat16)
        return jnp.dot(raised, values[spot(index), :], preferred_element_type=jnp.float32)

    scores = score(last)
    below = lax.broadcasted_iota(jnp.int32, scores.shape, 0) % tokens
    across = lax.broadcasted_iota(jnp.int32, scores.shape, 1)
    scores = jnp.where(across <= below + (mine % chunk_spans) * tokens, scores, masked_score)
    newest = top_of(scores)
    ahead[...] = score(0)
    total[...] = weigh(scores, newest, last)
    best[...] = newest

    def body(index, carry):
        scores = ahead[...]
        before = best[...]
        newest = jnp.maximum(before, top_of(scores))
        shrink = jnp.exp2(before - newest)
        ahead[...] = score(jnp.minimum(index + 1, last))
        update = weigh(scores, newest, index)
        total[...] = total[...] * jnp.concatenate([shrink] * 2, axis=1) + update
        best[...] = newest
        return carry

    lax.fori_loop(0, last, body, 0)
    for head in range(heads):
        lines = slice(head * tokens, (head + 1) * tokens)
        out_ref[0, :, head * HEAD_DIM : (head + 1) * HEAD_DIM] = (
            total[lines, :HEAD_DIM] / total[lines, HEAD_DIM:]
        ).astype(out_ref.dtype)


def attend(query, held, span_order, rows, cols):
    share = rows // KVHEADS
    tokens = query.shape[1]
    width = query.shape[2] // rows
    spans = span_order.shape[0]
    sequence = spans * tokens
    count = width // HEAD_DIM * tokens
    chunk_spans = 4
    return pl.pallas_call(
        functools.partial(attend_kernel, cols, share, chunk_spans),
        out_shape=jax.ShapeDtypeStruct((rows, tokens, width), query.dtype),
        grid_spec=pltpu.PrefetchScalarGridSpec(
            num_scalar_prefetch=1,
            grid=(rows,),
            in_specs=[
                pl.BlockSpec((1, tokens, width), lambda step, order: (step, 0, lax.axis_index("row"))),
                pl.BlockSpec(held.shape, lambda step, order: (0,) * held.ndim),
            ],
            out_specs=pl.BlockSpec((1, tokens, width), lambda step, order: (step, 0, 0)),
            scratch_shapes=[
                pltpu.VMEM((2 * HEAD_DIM, sequence), jnp.bfloat16),
                pltpu.VMEM((sequence, 2 * HEAD_DIM), jnp.bfloat16),
                pltpu.VMEM((count, 2 * HEAD_DIM), jnp.bfloat16),
                pltpu.VMEM((count, HEAD_DIM), jnp.float32),
                pltpu.VMEM((count, 2 * HEAD_DIM), jnp.float32),
                pltpu.VMEM((count, chunk_spans * tokens), jnp.float32),
            ],
        ),
        compiler_params=pltpu.CompilerParams(
            dimension_semantics=("arbitrary",), vmem_limit_bytes=VMEM_LIMIT
        ),
        name="attend",
    )(span_order, query, held)


def deliver_kernel(rows, part_ref, out_ref, own_sem, send_sem, recv_sem):
    row, col = lax.axis_index("row"), lax.axis_index("col")
    width = part_ref.shape[2]
    barrier = pltpu.get_barrier_semaphore()
    for step in range(1, rows):
        pl.semaphore_signal(
            barrier, inc=1, device_id=device(lax.rem(row + step, rows), col), device_id_type=MESH
        )
    pl.semaphore_wait(barrier, rows - 1)
    columns = pl.ds(pl.multiple_of(row * width, width), width)
    copies = []
    for step in range(1, rows):
        target = lax.rem(row + step, rows)
        copy = pltpu.make_async_remote_copy(
            src_ref=part_ref.at[target],
            dst_ref=out_ref.at[:, columns],
            send_sem=send_sem.at[step - 1],
            recv_sem=recv_sem.at[step - 1],
            device_id=device(target, col),
            device_id_type=MESH,
        )
        copy.start()
        copies.append(copy)
    own = pltpu.make_async_copy(part_ref.at[row], out_ref.at[:, columns], own_sem)
    own.start()
    own.wait()
    for copy in copies:
        copy.wait()


def deliver(parts):
    rows, tokens, width = parts.shape
    dma = pltpu.SemaphoreType.DMA
    return pl.pallas_call(
        functools.partial(deliver_kernel, rows),
        out_shape=jax.ShapeDtypeStruct((tokens, rows * width), parts.dtype),
        in_specs=[pl.BlockSpec(memory_space=pltpu.VMEM)],
        out_specs=pl.BlockSpec(memory_space=pl.ANY),
        scratch_shapes=[dma(()), dma((rows - 1,)), dma((rows - 1,))],
        compiler_params=pltpu.CompilerParams(
            collective_id=1, has_side_effects=True, vmem_limit_bytes=VMEM_LIMIT
        ),
        name="deliver",
    )(parts)


def shards(query, key, value, span_order):
    rows = lax.axis_size("row")
    cols = lax.axis_size("col")
    held = spread(key, value, rows, cols)
    parts = attend(query, held, span_order, rows, cols)
    return deliver(parts)


def solution(mesh):
    placed = (P(None, "col", None), P(("row", "col"), None), P(("row", "col"), None), P())
    return jax.shard_map(
        shards, mesh=mesh, in_specs=placed, out_specs=P(("row", "col"), None), check_vma=False
    )
```
